256 devices in a mesh: prow: 8 (over y, core), pcol: 32 (over x, z).
Axes of the slice: x: 4, y: 4, z: 8, core: 2. Of those that a mesh axis runs over, the one named last changes fastest.
Arguments:
- matrix: bfloat16 [2, 8, 8, 256, 2, 32, 256], P(None, None, 'prow', None, None, 'pcol'), may hold values from -6 to 6
Outputs:
- image: float32 [2, 8, 8, 256, 2, 32, 256], P(None, None, 'prow', None, None, 'pcol')
The draws below stay inside these ranges and needn't reach their ends.
All inputs are finite; a program needn't handle non-finite values.
Results may differ from the reference program's by a relative error of at most 0.0003.
Values sent between devices are 32-bit elements; how exact they have to be, the bound alone decides.
A program may use at most 64 MiB of HBM per device.

```python
import jax
import jax.numpy as jnp

IMAGES = 2
BLOCK = 256
ROW_BLOCKS = 8
COL_BLOCKS = 2
N_PROW = 8
N_PCOL = 32


def block_levels(key, extent, shards, low, high):
    loudness, own = 1.0, jax.random.fold_in(key, 6)
    for position, parts in shards:
        heights = jnp.exp(jax.random.uniform(jax.random.fold_in(own, position), (parts,), jnp.float32, low / len(shards), high / len(shards)))
        loudness = loudness * jnp.repeat(heights, extent[position] // parts).reshape([-1 if axis == position else 1 for axis in range(len(extent))])
    return loudness


def normal_values(stream_key, extent, spread, bound, split=(), kind=jnp.bfloat16):
    factor_of = block_levels(stream_key, extent, split, -0.22, 0.18) if split else 1.0
    result = jax.random.normal(stream_key, extent, jnp.float32) * spread * factor_of
    return jnp.minimum(jnp.maximum(result, -bound), bound).astype(kind)


def setup_inputs(seed: int = 0) -> dict:
    arg_keys = jax.random.split(jax.random.key(seed), 2)
    matrix = normal_values(arg_keys[0], (IMAGES, ROW_BLOCKS, N_PROW, BLOCK, COL_BLOCKS, N_PCOL, BLOCK), 1.0, 6.0, ((2, 8), (5, 32)))
    return {"matrix": matrix}


def reference(matrix):
    total_rows = ROW_BLOCKS * N_PROW * BLOCK
    total_cols = COL_BLOCKS * N_PCOL * BLOCK
    full = matrix.astype(jnp.float32).reshape(IMAGES, total_rows, total_cols)
    summed = jnp.cumsum(jnp.cumsum(full, axis=1, dtype=jnp.float32), axis=2, dtype=jnp.float32)
    row_factor = 1.0 / jnp.sqrt(jnp.arange(total_rows).astype(jnp.float32) + 1.0)
    col_factor = 1.0 / jnp.sqrt(jnp.arange(total_cols).astype(jnp.float32) + 1.0)
    scaled = summed * (row_factor[None, :, None] * col_factor[None, None, :])
    return scaled.reshape(IMAGES, ROW_BLOCKS, N_PROW, BLOCK, COL_BLOCKS, N_PCOL, BLOCK)
```

```python
import jax
import jax.numpy as jnp
from jax import lax
from jax.experimental import pallas as pl
from jax.experimental.pallas import tpu as pltpu
from jax.sharding import PartitionSpec as P

MESH = pl.DeviceIdType.MESH
F32, BF16 = jnp.float32, jnp.bfloat16
NI, NR, NC, B = 2, 8, 2, 256
NP, NX, NZ = 8, 4, 8
CHUNK = 4 * B
ROWS = NI * NR * CHUNK
BLOCKS = NI * NR * NC


def iota(shape, dim):
    return lax.broadcasted_iota(jnp.int32, shape, dim)


def dot(a, b, dims):
    return lax.dot_general(a, b, (dims, ((), ())), preferred_element_type=F32)


def split3(v):
    hi = v.astype(BF16)
    rest = v - hi.astype(F32)
    mid = rest.astype(BF16)
    low = (rest - mid.astype(F32)).astype(BF16)
    return hi, mid, low


def scan_kernel(
    x_hbm, l_ref, carry_ref, bt_ref,
    xv, fbuf, xb, rs, cs, tot, z1, x2, ca, ps, ts, tp, cp, vs, vz, vt, vx, cb,
    in_sem, z1_s, z1_r, x2_s, x2_r, ca_s, ca_r, tp_s, tp_r, cp_s, cp_r, vz_s, vz_r, vx_s, vx_r,
):
    p = lax.axis_index("prow")
    q = lax.axis_index("pcol")
    x, z = q // NZ, lax.rem(q, NZ)

    def z_mate(d):
        zz = lax.rem(z + d, NZ)
        return zz, (p, x * NZ + zz)

    def x_mate(d):
        xx = lax.rem(x + d, NX)
        return xx, (p, xx * NZ + z)

    def p_mate(d):
        pp = lax.rem(p + d, NP)
        return pp, (pp, q)

    z_order = (4, 3, 5, 2, 6, 1, 7)
    x_order = (2, 1, 3)
    p_order = (4, 5, 3, 2, 6, 7, 1)

    loads = []
    for r in range(NR):
        for n in range(NI):
            k = n * NR + r
            rows = pl.ds(k * CHUNK, CHUNK)
            copy = pltpu.make_async_copy(x_hbm.at[rows], xv.at[rows], in_sem.at[k])
            copy.start()
            loads.append(copy)

    barrier = pltpu.get_barrier_semaphore()
    for mate, order in ((z_mate, z_order), (x_mate, x_order), (p_mate, p_order)):
        for d in order:
            pl.semaphore_signal(barrier, inc=1, device_id=mate(d)[1], device_id_type=MESH)

    def copies(mate, order, src_of, dst, send, recv, me):
        out = []
        for d in order:
            other, device = mate(d)
            out.append(pltpu.make_async_remote_copy(
                src_ref=src_of(other), dst_ref=dst.at[me], send_sem=send.at[d], recv_sem=recv.at[me],
                device_id=device, device_id_type=MESH))
        return out

    def start(group):
        for c in group:
            c.start()

    def wait_recv(mate, order, src_of, dst, send, recv):
        for d in order:
            other, device = mate(d)
            pltpu.make_async_remote_copy(
                src_ref=src_of(other), dst_ref=dst.at[other], send_sem=send.at[d], recv_sem=recv.at[other],
                device_id=device, device_id_type=MESH).wait_recv()

    def wait_send(group):
        for c in group:
            c.wait_send()

    sub = iota((8, 128), 0)
    lane = iota((8, 128), 1)
    zero = jnp.zeros((8, 128), F32)
    row16 = iota((16, B), 0)
    one_hot = [jnp.where((row16 == k) | (row16 == k + 4), 1.0, 0.0).astype(BF16) for k in range(4)]

    totals = zero
    for r in range(NR):
        acc = jnp.zeros((16, B), F32)
        sums = []
        for n in range(NI):
            k = n * NR + r
            loads[r * NI + n].wait()
            f = xv[pl.ds(k * CHUNK, CHUNK), :].astype(F32)
            fbuf[n] = f
            s = jnp.sum(f.reshape(CHUNK // 64, 64, 128), axis=0)
            s = jnp.sum(s.reshape(8, 8, 128), axis=0)
            sums.append(s + pltpu.roll(s, 4, 0))
            for c in range(NC):
                left = fbuf[n, pl.ds(c, B, stride=4), :]
                right = fbuf[n, pl.ds(2 + c, B, stride=4), :]
                block = jnp.concatenate([left, right], axis=1).astype(BF16)
                xb[k * NC + c] = block
                acc += dot(one_hot[n * NC + c], block, ((1,), (1,)))
        rs[r] = jnp.where(sub < 4, acc[:8, :128], acc[:8, 128:])
        col = jnp.where(sub < 4, sums[0], sums[1])
        cs[r] = col
        totals = totals + jnp.where(lane == r, jnp.sum(col, axis=1, keepdims=True), 0.0)
    bt_bit = (sub // 2) % 2
    totals = totals + jnp.where(bt_bit == 0, pltpu.roll(totals, 6, 0), pltpu.roll(totals, 2, 0))
    tot[...] = totals
    z1[z] = rs[z]
    tp[p] = totals
    cp[p] = cs[...]

    pl.semaphore_wait(barrier, len(z_order) + len(x_order) + len(p_order))
    z1_src, tp_src, cp_src = (lambda o: rs.at[o]), (lambda o: tot), (lambda o: cs)
    z1_c = copies(z_mate, z_order, z1_src, z1, z1_s, z1_r, z)
    start(z1_c)
    tp_c = copies(p_mate, p_order, tp_src, tp, tp_s, tp_r, p)
    start(tp_c)
    cp_c = copies(p_mate, p_order, cp_src, cp, cp_s, cp_r, p)
    start(cp_c)

    upper = jnp.where(iota((B, B), 0) <= iota((B, B), 1), 1.0, 0.0).astype(BF16)
    lower = jnp.where(iota((B, B), 1) <= iota((B, B), 0), 1.0, 0.0).astype(BF16)

    def local_prefix(first, last):
        def body(i, _):
            u = dot(xb[i], upper, ((1,), (0,)))
            hi = u.astype(BF16)
            low = (u - hi.astype(F32)).astype(BF16)
            l_ref[pl.ds(i * B, B), :] = dot(lower, hi, ((1,), (0,))) + dot(lower, low, ((1,), (0,)))
            return 0
        lax.fori_loop(first, last, body, 0)

    local_prefix(0, 6)

    wait_recv(p_mate, p_order, tp_src, tp, tp_s, tp_r)
    every, before = zero, zero
    for i in range(NP):
        t = tp[i]
        every = every + t
        before = before + jnp.where(i < p, t, 0.0)
    for step in (1, 2, 4):
        every = every + jnp.where(lane >= step, pltpu.roll(every, step, 1), 0.0)
    v = before + jnp.where(lane >= 1, pltpu.roll(every, 1, 1), 0.0)
    vs[...] = v
    vz[z] = v
    vz_src = lambda o: vs
    vz_c = copies(z_mate, z_order, vz_src, vz, vz_s, vz_r, z)
    start(vz_c)

    local_prefix(6, 10)

    wait_recv(z_mate, z_order, z1_src, z1, z1_s, z1_r)
    run = zero
    prefix = []
    for i in range(NZ):
        prefix.append(run)
        run = run + z1[i]
    ts[...] = run
    x2[x] = run
    x2_src = lambda o: ts
    x2_c = copies(x_mate, x_order, x2_src, x2, x2_s, x2_r, x)
    start(x2_c)
    for i in range(NZ):
        ps[i] = prefix[i]

    local_prefix(10, 16)

    c_bit = sub % 2

    def x_base(ref):
        every, before = zero, zero
        for i in range(NX):
            t = ref[i]
            every = every + t
            before = before + jnp.where(i < x, t, 0.0)
        return before + jnp.where(c_bit == 1, pltpu.roll(every, 1, 0), 0.0)

    wait_recv(x_mate, x_order, x2_src, x2, x2_s, x2_r)
    base = x_base(x2)
    for i in range(NZ):
        ps[i] = ps[i] + base
    ca[z] = ps[z]
    ca_src = lambda o: ps.at[o]
    ca_c = copies(z_mate, z_order, ca_src, ca, ca_s, ca_r, z)
    start(ca_c)

    wait_recv(z_mate, z_order, vz_src, vz, vz_s, vz_r)
    every, before = zero, zero
    for i in range(NZ):
        t = vz[i]
        every = every + t
        before = before + jnp.where(i < z, t, 0.0)
    vt[...] = every
    vx[x] = every
    vx_src = lambda o: vt
    vx_c = copies(x_mate, x_order, vx_src, vx, vx_s, vx_r, x)
    start(vx_c)

    local_prefix(16, 22)

    wait_recv(p_mate, p_order, cp_src, cp, cp_s, cp_r)
    run = zero
    for r in range(NR):
        above = zero
        step = zero
        for i in range(NP):
            t = cp[i, r]
            step = step + t
            above = above + jnp.where(i < p, t, 0.0)
        cb[r] = run + above
        run = run + step
    half = jnp.where((iota((128, B), 0) <= iota((128, B), 1)), 1.0, 0.0).astype(BF16)
    scans = jnp.zeros((8 * NR, B), F32)
    for part in split3(cb[...].reshape(8 * NR, 128)):
        scans = scans + dot(part, half, ((1,), (0,)))
    cb[...] = scans[:, :128].reshape(NR, 8, 128)
    bt_ref[...] = scans[:, 128:].reshape(NR, 8, 128)
    for r in range(NR):
        cb[r] = cb[r] + jnp.where(bt_bit == 1, pltpu.roll(bt_ref[r], 2, 0), 0.0)

    local_prefix(22, BLOCKS)

    wait_recv(x_mate, x_order, vx_src, vx, vx_s, vx_r)
    corner = before + x_base(vx)
    for r in range(NR):
        bt_ref[r] = cb[r] + jnp.sum(jnp.where(lane == r, corner, 0.0), axis=1, keepdims=True)

    wait_recv(z_mate, z_order, ca_src, ca, ca_s, ca_r)
    carry_ref[...] = ca[...].reshape(8 * NR, 128)
    for group in (z1_c, tp_c, cp_c, vz_c, x2_c, ca_c, vx_c):
        wait_send(group)


def write_kernel(l_ref, carry_ref, bt_ref, o_hbm, at, stage, sem):
    p = lax.axis_index("prow")
    q = lax.axis_index("pcol")
    lower = jnp.where(iota((B, B), 1) <= iota((B, B), 0), 1.0, 0.0).astype(BF16)
    near = jnp.zeros((B, 8 * NR), F32)
    far = jnp.zeros((B, 8 * NR), F32)
    for part in split3(carry_ref[...]):
        near = near + dot(lower[:, :128], part, ((1,), (1,)))
        far = far + dot(lower[:, 128:], part, ((1,), (1,)))
    at[...] = near + pltpu.roll(far, 8 * NR - 4, 1)

    T = 64
    outs = []
    cf = [[lax.rsqrt(((c * NX * NZ + q) * B + bt * 128 + 1 + iota((1, 128), 1)).astype(F32)) for bt in range(2)] for c in range(NC)]
    for r in range(NR):
        for t in range(B // T):
            rf = lax.rsqrt(((r * NP + p) * B + t * T + 1 + iota((T, 128), 0)).astype(F32))
            for n in range(NI):
                k = n * NR + r
                for c in range(NC):
                    col = r * 8 + n * NC + c
                    av = jnp.broadcast_to(at[pl.ds(t * T, T), col:col + 1], (T, 128))
                    for bt in range(2):
                        bv = bt_ref[r, pl.ds(n * 4 + bt * 2 + c, 1), :]
                        lv = l_ref[pl.ds((k * NC + c) * B + t * T, T), pl.ds(bt * 128, 128)]
                        stage[pl.ds(k * CHUNK + t * T * 4 + c * 2 + bt, T, stride=4), :] = (lv + (av + bv)) * (rf * cf[c][bt])
        for n in range(NI):
            k = n * NR + r
            rows = pl.ds(k * CHUNK, CHUNK)
            copy = pltpu.make_async_copy(stage.at[rows], o_hbm.at[rows], sem.at[k])
            copy.start()
            outs.append(copy)
    for copy in outs:
        copy.wait()


def shards(matrix):
    rows = matrix.reshape(NI, NR, B, NC, 2, 128).transpose(0, 1, 2, 4, 3, 5).reshape(ROWS, 128)
    rows = pltpu.with_memory_space_constraint(rows, pltpu.HBM)
    hbm = pl.BlockSpec(memory_space=pltpu.HBM)
    vmem = pl.BlockSpec(memory_space=pltpu.VMEM)
    dma = pltpu.SemaphoreType.DMA
    tile = lambda *lead: pltpu.VMEM((*lead, 8, 128), F32)
    local, carry, bt = pl.pallas_call(
        scan_kernel,
        out_shape=(
            pltpu.VMEM((BLOCKS * B, B), F32),
            pltpu.VMEM((8 * NR, 128), F32),
            pltpu.VMEM((NR, 8, 128), F32),
        ),
        in_specs=[hbm],
        out_specs=(vmem, vmem, vmem),
        scratch_shapes=[
            pltpu.VMEM((ROWS, 128), BF16),
            pltpu.VMEM((NI, CHUNK, 128), F32),
            pltpu.VMEM((BLOCKS, B, B), BF16),
            tile(NR), tile(NR), tile(),
            tile(NZ), tile(NX), tile(NZ), tile(NZ), tile(),
            tile(NP), tile(NP, NR), tile(), tile(NZ), tile(), tile(NX), tile(NR),
            dma((NI * NR,)),
            dma((NZ,)), dma((NZ,)), dma((NX,)), dma((NX,)), dma((NZ,)), dma((NZ,)),
            dma((NP,)), dma((NP,)), dma((NP,)), dma((NP,)), dma((NZ,)), dma((NZ,)), dma((NX,)), dma((NX,)),
        ],
        compiler_params=pltpu.CompilerParams(collective_id=0, has_side_effects=True, vmem_limit_bytes=24 << 20),
        name="scan",
    )(rows)
    out = pl.pallas_call(
        write_kernel,
        out_shape=pltpu.HBM((ROWS, 128), F32),
        in_specs=[vmem, vmem, vmem],
        out_specs=hbm,
        scratch_shapes=[pltpu.VMEM((B, 8 * NR), F32), pltpu.VMEM((ROWS, 128), F32), dma((NI * NR,))],
        compiler_params=pltpu.CompilerParams(vmem_limit_bytes=24 << 20),
        name="write",
    )(local, carry, bt)
    return out.reshape(NI, NR, 1, B, NC, 1, B)


def solution(mesh):
    return jax.shard_map(
        shards,
        mesh=mesh,
        in_specs=(P(None, None, "prow", None, None, "pcol", None),),
        out_specs=P(None, None, "prow", None, None, "pcol", None),
        check_vma=False,
    )
```

```python
import jax
import jax.numpy as jnp
from jax import lax
from jax.experimental import pallas as pl
from jax.experimental.pallas import tpu as pltpu
from jax.sharding import PartitionSpec as P

MESH = pl.DeviceIdType.MESH
F32, BF16 = jnp.float32, jnp.bfloat16
NI, NR, NC, B = 2, 8, 2, 256
NP, NX, NZ = 8, 4, 8
CHUNK = 4 * B
ROWS = NI * NR * CHUNK
BLOCKS = NI * NR * NC
SEG, PAD = CHUNK // 8, CHUNK // 8 + 8
STEPS = B // 8
GROUPS = 4


def iota(shape, dim):
    return lax.broadcasted_iota(jnp.int32, shape, dim)


def dot(a, b, dims):
    return lax.dot_general(a, b, (dims, ((), ())), preferred_element_type=F32)


def split3(v):
    hi = v.astype(BF16)
    rest = v - hi.astype(F32)
    mid = rest.astype(BF16)
    low = (rest - mid.astype(F32)).astype(BF16)
    return hi, mid, low


def rows_before(v):
    row = iota(v.shape, v.ndim - 2)
    for step in (1, 2, 4):
        v = v + jnp.where(row >= step, pltpu.roll(v, step, v.ndim - 2), 0.0)
    return jnp.where(row >= 1, pltpu.roll(v, 1, v.ndim - 2), 0.0)


def scan_kernel(
    x_hbm, l_ref, e_ref, carry_ref, bt_ref,
    xv, fbuf, rs, cs, tot, z1, x2, ca, ps, ts, tp, cp, vs, vz, vt, vx, cb,
    in_sem, send_sem, z1_r, x2_r, ca_r, tp_r, cp_r, vz_r, vx_r,
):
    p = lax.axis_index("prow")
    q = lax.axis_index("pcol")
    x, z = q // NZ, lax.rem(q, NZ)

    def z_mate(d):
        zz = lax.rem(z + d, NZ)
        return zz, (p, x * NZ + zz)

    def x_mate(d):
        xx = lax.rem(x + d, NX)
        return xx, (p, xx * NZ + z)

    def p_mate(d):
        pp = lax.rem(p + d, NP)
        return pp, (pp, q)

    z_order = (4, 3, 5, 2, 6, 1, 7)
    x_order = (2, 1, 3)
    p_order = (4, 5, 3, 2, 6, 7, 1)

    part = NR // GROUPS
    for g in range(GROUPS):
        for n in range(NI):
            rows = pl.ds((n * NR + g * part) * CHUNK, part * CHUNK)
            pltpu.make_async_copy(x_hbm.at[rows], xv.at[rows], in_sem.at[g]).start()

    barrier = pltpu.get_barrier_semaphore()
    for mate, order in ((z_mate, z_order), (x_mate, x_order), (p_mate, p_order)):
        for d in order:
            pl.semaphore_signal(barrier, inc=1, device_id=mate(d)[1], device_id_type=MESH)

    def send(mate, order, src_of, dst, recv, me):
        for d in order:
            other, device = mate(d)
            pltpu.make_async_remote_copy(
                src_ref=src_of(other), dst_ref=dst.at[me], send_sem=send_sem.at[0], recv_sem=recv.at[0],
                device_id=device, device_id_type=MESH).start()

    def receive(mate, order, dst, recv):
        every = dst.at[pl.ds(0, len(order))]
        pltpu.make_async_remote_copy(
            src_ref=every, dst_ref=every, send_sem=send_sem.at[0], recv_sem=recv.at[0],
            device_id=mate(1)[1], device_id_type=MESH).wait_recv()

    sub = iota((8, 128), 0)
    lane = iota((8, 128), 1)
    zero = jnp.zeros((8, 128), F32)
    row16, col16 = iota((16, B), 0), iota((16, B), 1)
    pick = [jnp.where((row16 // 8 == col16 // 128) & (row16 % 8 // 2 == t), 1.0, 0.0).astype(BF16) for t in range(4)]

    totals = zero
    for g in range(GROUPS):
      with jax.named_scope(f"sums{g}"):
        rows = pl.ds(g * NI * part * CHUNK, NI * part * CHUNK)
        pltpu.make_async_copy(x_hbm.at[rows], xv.at[rows], in_sem.at[g]).wait()
        for r in range(g * part, (g + 1) * part):
            acc = jnp.zeros((16, B), F32)
            for t in range(4):
                pair = [xv[pl.ds((n * NR + r) * CHUNK + t * B, B), :] for n in range(NI)]
                acc = acc + dot(pick[t], jnp.concatenate(pair, axis=1), ((1,), (1,)))
            sums = []
            for n in range(NI):
                f = xv[pl.ds((n * NR + r) * CHUNK, CHUNK), :].astype(F32)
                s = jnp.sum(f.reshape(CHUNK // 64, 64, 128), axis=0)
                s = jnp.sum(s.reshape(8, 8, 128), axis=0)
                sums.append(s + pltpu.roll(s, 4, 0))
            one, two = [jnp.where(sub % 2 == 0, acc[n * 8:n * 8 + 8, :128], acc[n * 8:n * 8 + 8, 128:]) for n in range(NI)]
            rs[r] = jnp.where(lane // 2 % 2 == 0, one + pltpu.roll(one, 126, 1), two + pltpu.roll(two, 2, 1))
            col = jnp.where(sub < 4, sums[0], sums[1])
            cs[r] = col
            totals = totals + jnp.where(lane == r, jnp.sum(col, axis=1, keepdims=True), 0.0)
    bt_bit = sub // 2 % 2
    totals = totals + jnp.where(bt_bit == 0, pltpu.roll(totals, 6, 0), pltpu.roll(totals, 2, 0))
    tot[...] = totals
    z1[z] = rs[z]
    tp[p] = totals
    cp[p] = cs[...]

    with jax.named_scope("barrier"):
        pl.semaphore_wait(barrier, len(z_order) + len(x_order) + len(p_order))
    send(z_mate, z_order, lambda o: rs.at[o], z1, z1_r, z)
    send(p_mate, p_order, lambda o: tot, tp, tp_r, p)
    send(p_mate, p_order, lambda o: cs, cp, cp_r, p)

    upper = jnp.where(iota((B, B), 0) <= iota((B, B), 1), 1.0, 0.0).astype(BF16)

    def local_prefix(first, last):
        def body(i, _):
            tiles = []
            for h in range(2):
                k = i * 2 + h
                for s in range(8):
                    fbuf[h, pl.ds(s * PAD, SEG), :] = xv[pl.ds(k * CHUNK + s * SEG, SEG), :].astype(F32)
                for c in range(NC):
                    halves = [jnp.concatenate([fbuf[h, pl.ds(j * 4 + bt * 2 + c, 8, stride=PAD), :] for j in range(STEPS)], axis=0) for bt in range(2)]
                    tiles.append((k * NC + c, jnp.concatenate(halves, axis=1).astype(BF16)))
            scans = [(b, dot(v, upper, ((1,), (0,)))) for b, v in tiles]
            for b, u in scans:
                run = jnp.zeros((8, B), F32)
                for j in range(STEPS):
                    run = run + u[j * 8:j * 8 + 8]
                    l_ref[pl.ds(b * B + j * 8, 8), :] = run
                e_ref[b] = rows_before(run)
            return 0
        with jax.named_scope(f"lp{first}"):
            lax.fori_loop(first, last, body, 0)

    local_prefix(0, 2)

    with jax.named_scope("wait_tp"):
        receive(p_mate, p_order, tp, tp_r)
    every, before = zero, zero
    for i in range(NP):
        t = tp[i]
        every = every + t
        before = before + jnp.where(i < p, t, 0.0)
    for step in (1, 2, 4):
        every = every + jnp.where(lane >= step, pltpu.roll(every, step, 1), 0.0)
    v = before + jnp.where(lane >= 1, pltpu.roll(every, 1, 1), 0.0)
    vs[...] = v
    vz[z] = v
    send(z_mate, z_order, lambda o: vs, vz, vz_r, z)

    local_prefix(2, 4)

    with jax.named_scope("wait_z1"):
        receive(z_mate, z_order, z1, z1_r)
    run = zero
    for i in range(NZ):
        ps[i] = run
        run = run + z1[i]
    ts[...] = run
    x2[x] = run
    send(x_mate, x_order, lambda o: ts, x2, x2_r, x)

    local_prefix(4, 6)

    def x_base(ref, axis, bit):
        every, before = zero, zero
        for i in range(NX):
            t = ref[i]
            every = every + t
            before = before + jnp.where(i < x, t, 0.0)
        return before + jnp.where(bit == 1, pltpu.roll(every, 1, axis), 0.0)

    with jax.named_scope("wait_x2"):
        receive(x_mate, x_order, x2, x2_r)
    base = x_base(x2, 1, lane % 2)
    for i in range(NZ):
        ps[i] = ps[i] + base
    ca[z] = ps[z]
    send(z_mate, z_order, lambda o: ps.at[o], ca, ca_r, z)

    with jax.named_scope("wait_vz"):
        receive(z_mate, z_order, vz, vz_r)
    every, before = zero, zero
    for i in range(NZ):
        t = vz[i]
        every = every + t
        before = before + jnp.where(i < z, t, 0.0)
    vt[...] = every
    vx[x] = every
    send(x_mate, x_order, lambda o: vt, vx, vx_r, x)

    local_prefix(6, 7)

    with jax.named_scope("wait_cp"):
        receive(p_mate, p_order, cp, cp_r)
    run = zero
    for r in range(NR):
        above, step = zero, zero
        for i in range(NP):
            t = cp[i, r]
            step = step + t
            above = above + jnp.where(i < p, t, 0.0)
        cb[r] = run + above
        run = run + step
    half = jnp.where(iota((128, B), 0) <= iota((128, B), 1), 1.0, 0.0).astype(BF16)
    scans = jnp.zeros((8 * NR, B), F32)
    for piece in split3(cb[...].reshape(8 * NR, 128)):
        scans = scans + dot(piece, half, ((1,), (0,)))
    cb[...] = scans[:, :128].reshape(NR, 8, 128)
    bt_ref[...] = scans[:, 128:].reshape(NR, 8, 128)
    for r in range(NR):
        cb[r] = cb[r] + jnp.where(bt_bit == 1, pltpu.roll(bt_ref[r], 2, 0), 0.0)

    local_prefix(7, 8)

    with jax.named_scope("wait_vx"):
        receive(x_mate, x_order, vx, vx_r)
    corner = before + x_base(vx, 0, sub % 2)
    for r in range(NR):
        bt_ref[r] = cb[r] + jnp.sum(jnp.where(lane == r, corner, 0.0), axis=1, keepdims=True)

    with jax.named_scope("wait_ca"):
        receive(z_mate, z_order, ca, ca_r)
    carry_ref[...] = ca[...].reshape(8 * NR, 128)
    tiles = 3 * len(z_order) + 2 * len(x_order) + (1 + NR) * len(p_order)
    sent = l_ref.at[pl.ds(0, tiles * 8 // 2)]
    with jax.named_scope("wait_send"):
        pltpu.make_async_remote_copy(
            src_ref=sent, dst_ref=sent, send_sem=send_sem.at[0], recv_sem=z1_r.at[0],
            device_id=z_mate(1)[1], device_id_type=MESH).wait_send()


def write_kernel(l_ref, e_ref, carry_ref, bt_ref, o_hbm, av, stage, sem):
    p = lax.axis_index("prow")
    q = lax.axis_index("pcol")
    src, dst = iota((128, B), 0), iota((128, B), 1)
    near = jnp.where((src % 4 == dst % 4) & ((src // 4 <= dst // 4) | (dst >= 128)), 1.0, 0.0).astype(BF16)
    scans = jnp.zeros((8 * NR, B), F32)
    for piece in split3(carry_ref[...]):
        scans = scans + dot(piece, near, ((1,), (0,)))
    av[...] = scans[:, :128].reshape(NR, 8, 128) + rows_before(scans[:, 128:].reshape(NR, 8, 128))

    cf = [[lax.rsqrt(((c * NX * NZ + q) * B + bt * 128 + 1 + iota((8, 128), 1)).astype(F32)) for bt in range(2)] for c in range(NC)]
    first_row = (p * B + 1 + iota((8, 128), 0) * STEPS).astype(F32)
    for r in range(NR):
        carry = av[r]
        offset = {}
        for n in range(NI):
            for c in range(NC):
                for bt in range(2):
                    own = e_ref[(n * NR + r) * NC + c][:, bt * 128:bt * 128 + 128]
                    offset[n, c, bt] = own + bt_ref[r, pl.ds(n * 4 + bt * 2 + c, 1), :]
        for j in range(STEPS):
            rf = lax.rsqrt(first_row + float(r * NP * B + j))
            scale = [[rf * cf[c][bt] for bt in range(2)] for c in range(NC)]
            for n in range(NI):
                k = n * NR + r
                for c in range(NC):
                    at = j * 4 + n * 2 + c
                    a = jnp.broadcast_to(carry[:, at:at + 1], (8, 128))
                    for bt in range(2):
                        lv = l_ref[pl.ds((k * NC + c) * B + j * 8, 8), pl.ds(bt * 128, 128)]
                        stage[pl.ds(k * 8 * PAD + j * 4 + c * 2 + bt, 8, stride=PAD), :] = (lv + (a + offset[n, c, bt])) * scale[c][bt]
        for n in range(NI):
            k = n * NR + r
            for s in range(8):
                pltpu.make_async_copy(
                    stage.at[pl.ds((k * 8 + s) * PAD, SEG)], o_hbm.at[pl.ds((k * 8 + s) * SEG, SEG)], sem.at[0]).start()
    pltpu.make_async_copy(stage.at[pl.ds(0, ROWS)], o_hbm, sem.at[0]).wait()


def shards(matrix):
    rows = matrix.reshape(NI, NR, B, NC, 2, 128).transpose(0, 1, 2, 4, 3, 5).reshape(ROWS, 128)
    rows = pltpu.with_memory_space_constraint(rows, pltpu.HBM)
    hbm = pl.BlockSpec(memory_space=pltpu.HBM)
    vmem = pl.BlockSpec(memory_space=pltpu.VMEM)
    dma = pltpu.SemaphoreType.DMA
    tile = lambda *lead: pltpu.VMEM((*lead, 8, 128), F32)
    found = pl.pallas_call(
        scan_kernel,
        out_shape=(
            pltpu.VMEM((BLOCKS * B, B), F32),
            pltpu.VMEM((BLOCKS, 8, B), F32),
            pltpu.VMEM((8 * NR, 128), F32),
            pltpu.VMEM((NR, 8, 128), F32),
        ),
        in_specs=[hbm],
        out_specs=(vmem, vmem, vmem, vmem),
        scratch_shapes=[
            pltpu.VMEM((ROWS, 128), BF16),
            pltpu.VMEM((2, 8 * PAD, 128), F32),
            tile(NR), tile(NR), tile(),
            tile(NZ), tile(NX), tile(NZ), tile(NZ), tile(),
            tile(NP), tile(NP, NR), tile(), tile(NZ), tile(), tile(NX), tile(NR),
            dma((GROUPS,)),
        ] + [dma((1,))] * 8,
        compiler_params=pltpu.CompilerParams(collective_id=0, has_side_effects=True, vmem_limit_bytes=24 << 20),
        name="scan",
    )(rows)
    out = pl.pallas_call(
        write_kernel,
        out_shape=pltpu.HBM((ROWS, 128), F32),
        in_specs=[vmem, vmem, vmem, vmem],
        out_specs=hbm,
        scratch_shapes=[tile(NR), pltpu.VMEM((NI * NR * 8 * PAD, 128), F32), dma((1,))],
        compiler_params=pltpu.CompilerParams(vmem_limit_bytes=24 << 20),
        name="write",
    )(*found)
    return out.reshape(NI, NR, 1, B, NC, 1, B)


def solution(mesh):
    return jax.shard_map(
        shards,
        mesh=mesh,
        in_specs=(P(None, None, "prow", None, None, "pcol", None),),
        out_specs=P(None, None, "prow", None, None, "pcol", None),
        check_vma=False,
    )
```

```python
import jax
import jax.numpy as jnp
from jax import lax
from jax.experimental import pallas as pl
from jax.experimental.pallas import tpu as pltpu
from jax.sharding import PartitionSpec as P

MESH = pl.DeviceIdType.MESH
F32, BF16 = jnp.float32, jnp.bfloat16
NI, NR, NC, B = 2, 8, 2, 256
NP, NX, NZ = 8, 4, 8
CHUNK = 4 * B
ROWS = NI * NR * CHUNK
BLOCKS = NI * NR * NC
SEG, PAD = CHUNK // 8, CHUNK // 8 + 8
STEPS = B // 8
GROUPS = 4


def iota(shape, dim):
    return lax.broadcasted_iota(jnp.int32, shape, dim)


def dot(a, b, dims):
    return lax.dot_general(a, b, (dims, ((), ())), preferred_element_type=F32)


def split3(v):
    hi = v.astype(BF16)
    rest = v - hi.astype(F32)
    mid = rest.astype(BF16)
    low = (rest - mid.astype(F32)).astype(BF16)
    return hi, mid, low


def rows_before(v):
    row = iota(v.shape, v.ndim - 2)
    for step in (1, 2, 4):
        v = v + jnp.where(row >= step, pltpu.roll(v, step, v.ndim - 2), 0.0)
    return jnp.where(row >= 1, pltpu.roll(v, 1, v.ndim - 2), 0.0)


def scan_kernel(
    x_hbm, l_ref, e_ref, carry_ref, bt_ref,
    xv, fbuf, rs, cs, tot, z1, x2, ca, ps, ts, tp, cp, vs, vq, cb,
    in_sem, send_sem, vq_s, z1_r, x2_r, ca_r, tp_r, cp_r, vq_r,
):
    p = lax.axis_index("prow")
    q = lax.axis_index("pcol")
    x, z = q // NZ, lax.rem(q, NZ)

    def z_mate(d):
        zz = lax.rem(z + d, NZ)
        return zz, (p, x * NZ + zz)

    def x_mate(d):
        xx = lax.rem(x + d, NX)
        return xx, (p, xx * NZ + z)

    def p_mate(d):
        pp = lax.rem(p + d, NP)
        return pp, (pp, q)

    def q_mate(d):
        qq = lax.rem(x + d[0], NX) * NZ + lax.rem(z + d[1], NZ)
        return qq, (p, qq)

    z_order = (4, 3, 5, 2, 6, 1, 7)
    x_order = (2, 1, 3)
    p_order = (4, 5, 3, 2, 6, 7, 1)
    hops = lambda d: min(d[0], NX - d[0]) + min(d[1], NZ - d[1])
    q_order = sorted([(a, b) for a in range(NX) for b in range(NZ) if a or b], key=hops, reverse=True)

    part = NR // GROUPS
    for g in range(GROUPS):
        for n in range(NI):
            rows = pl.ds((n * NR + g * part) * CHUNK, part * CHUNK)
            pltpu.make_async_copy(x_hbm.at[rows], xv.at[rows], in_sem.at[g]).start()

    barrier = pltpu.get_barrier_semaphore()
    for mate, order in ((z_mate, z_order), (x_mate, x_order), (p_mate, p_order)):
        for d in order:
            pl.semaphore_signal(barrier, inc=1, device_id=mate(d)[1], device_id_type=MESH)

    def send(mate, order, src_of, dst, recv, me, sent=send_sem):
        for d in order:
            other, device = mate(d)
            pltpu.make_async_remote_copy(
                src_ref=src_of(other), dst_ref=dst.at[me], send_sem=sent.at[0], recv_sem=recv.at[0],
                device_id=device, device_id_type=MESH).start()

    def receive(mate, order, dst, recv):
        every = dst.at[pl.ds(0, len(order))]
        pltpu.make_async_remote_copy(
            src_ref=every, dst_ref=every, send_sem=send_sem.at[0], recv_sem=recv.at[0],
            device_id=mate(order[0])[1], device_id_type=MESH).wait_recv()

    sub = iota((8, 128), 0)
    lane = iota((8, 128), 1)
    zero = jnp.zeros((8, 128), F32)
    row16, col16 = iota((16, B), 0), iota((16, B), 1)
    pick = [jnp.where((row16 // 8 == col16 // 128) & (row16 % 8 // 2 == t), 1.0, 0.0).astype(BF16) for t in range(4)]

    totals = zero
    for g in range(GROUPS):
      with jax.named_scope(f"sums{g}"):
        rows = pl.ds(g * NI * part * CHUNK, NI * part * CHUNK)
        pltpu.make_async_copy(x_hbm.at[rows], xv.at[rows], in_sem.at[g]).wait()
        for r in range(g * part, (g + 1) * part):
            acc = jnp.zeros((16, B), F32)
            for t in range(4):
                pair = [xv[pl.ds((n * NR + r) * CHUNK + t * B, B), :] for n in range(NI)]
                acc = acc + dot(pick[t], jnp.concatenate(pair, axis=1), ((1,), (1,)))
            sums = []
            for n in range(NI):
                f = xv[pl.ds((n * NR + r) * CHUNK, CHUNK), :].astype(F32)
                s = jnp.sum(f.reshape(CHUNK // 64, 64, 128), axis=0)
                s = jnp.sum(s.reshape(8, 8, 128), axis=0)
                sums.append(s + pltpu.roll(s, 4, 0))
            one, two = [jnp.where(sub % 2 == 0, acc[n * 8:n * 8 + 8, :128], acc[n * 8:n * 8 + 8, 128:]) for n in range(NI)]
            rs[r] = jnp.where(lane // 2 % 2 == 0, one + pltpu.roll(one, 126, 1), two + pltpu.roll(two, 2, 1))
            col = jnp.where(sub < 4, sums[0], sums[1])
            cs[r] = col
            here = (lane == NR + r) | ((lane > r) & (lane < NR))
            totals = totals + jnp.where(here, jnp.sum(col, axis=1, keepdims=True), 0.0)
    bt_bit = sub // 2 % 2
    tot[...] = totals
    z1[z] = rs[z]
    tp[p] = totals
    cp[p] = cs[...]

    with jax.named_scope("barrier"):
        pl.semaphore_wait(barrier, len(z_order) + len(x_order) + len(p_order))
    send(z_mate, z_order, lambda o: rs.at[o], z1, z1_r, z)
    send(p_mate, p_order, lambda o: tot, tp, tp_r, p)
    send(p_mate, p_order, lambda o: cs, cp, cp_r, p)

    upper = jnp.where(iota((B, B), 0) <= iota((B, B), 1), 1.0, 0.0).astype(BF16)

    def local_prefix(first, last):
        def body(i, _):
            tiles = []
            for h in range(2):
                k = i * 2 + h
                for s in range(8):
                    fbuf[h, pl.ds(s * PAD, SEG), :] = xv[pl.ds(k * CHUNK + s * SEG, SEG), :].astype(F32)
                for c in range(NC):
                    halves = [jnp.concatenate([fbuf[h, pl.ds(j * 4 + bt * 2 + c, 8, stride=PAD), :] for j in range(STEPS)], axis=0) for bt in range(2)]
                    tiles.append((k * NC + c, jnp.concatenate(halves, axis=1).astype(BF16)))
            scans = [(b, dot(v, upper, ((1,), (0,)))) for b, v in tiles]
            for b, u in scans:
                run = jnp.zeros((8, B), F32)
                for j in range(STEPS):
                    run = run + u[j * 8:j * 8 + 8]
                    l_ref[pl.ds(b * B + j * 8, 8), :] = run
                e_ref[b] = rows_before(run)
            return 0
        with jax.named_scope(f"lp{first}"):
            lax.fori_loop(first, last, body, 0)

    local_prefix(0, 4)

    with jax.named_scope("wait_z1"):
        receive(z_mate, z_order, z1, z1_r)
    run = zero
    for i in range(NZ):
        ps[i] = run
        run = run + z1[i]
    ts[...] = run
    x2[x] = run
    send(x_mate, x_order, lambda o: ts, x2, x2_r, x)

    with jax.named_scope("wait_tp"):
        receive(p_mate, p_order, tp, tp_r)
    every, before = zero, zero
    for i in range(NP):
        t = tp[i]
        every = every + t
        before = before + jnp.where(i < p, t, 0.0)
    v = every + pltpu.roll(before, 128 - NR, 1)
    v = pltpu.roll(v, 0, 1, stride=NR, stride_axis=0)
    v = jnp.sum(jnp.where(lane // NR == sub, v, 0.0), axis=0, keepdims=True)
    vs[0] = v
    vq[q] = v
    send(q_mate, q_order, lambda o: vs.at[0], vq, vq_r, q, vq_s)

    local_prefix(4, 7)

    with jax.named_scope("wait_x2"):
        receive(x_mate, x_order, x2, x2_r)
    every, before = zero, zero
    for i in range(NX):
        t = x2[i]
        every = every + t
        before = before + jnp.where(i < x, t, 0.0)
    base = before + jnp.where(lane % 2 == 1, pltpu.roll(every, 1, 1), 0.0)
    for i in range(NZ):
        ps[i] = ps[i] + base
    ca[z] = ps[z]
    send(z_mate, z_order, lambda o: ps.at[o], ca, ca_r, z)

    local_prefix(7, 8)

    with jax.named_scope("wait_cp"):
        receive(p_mate, p_order, cp, cp_r)
    run = zero
    for r in range(NR):
        above, step = zero, zero
        for i in range(NP):
            t = cp[i, r]
            step = step + t
            above = above + jnp.where(i < p, t, 0.0)
        cb[r] = run + above
        run = run + step
    half = jnp.where(iota((128, B), 0) <= iota((128, B), 1), 1.0, 0.0).astype(BF16)
    scans = jnp.zeros((8 * NR, B), F32)
    for piece in split3(cb[...].reshape(8 * NR, 128)):
        scans = scans + dot(piece, half, ((1,), (0,)))
    cb[...] = scans[:, :128].reshape(NR, 8, 128)
    bt_ref[...] = scans[:, 128:].reshape(NR, 8, 128)
    for r in range(NR):
        cb[r] = cb[r] + jnp.where(bt_bit == 1, pltpu.roll(bt_ref[r], 2, 0), 0.0)

    with jax.named_scope("wait_vq"):
        receive(q_mate, q_order, vq, vq_r)
    every, before = [0.0] * 4, [0.0] * 4
    for i in range(NX * NZ):
        t = vq[i]
        every[i % 4] = every[i % 4] + t
        before[i % 4] = before[i % 4] + jnp.where(i < q, t, 0.0)
    every, before = [(t[0] + t[1]) + (t[2] + t[3]) for t in (every, before)]
    every, before = [jnp.broadcast_to(t, (8, 128)) for t in (every, before)]
    corner = before + jnp.where(lane // NR % 2 == 1, pltpu.roll(every, NR, 1), 0.0)
    corner = jnp.where(lane // NR // 4 * 2 + lane // NR % 2 == sub // 4 * 2 + sub % 2, corner, 0.0)
    for r in range(NR):
        bt_ref[r] = cb[r] + jnp.sum(jnp.where(lane % NR == r, corner, 0.0), axis=1, keepdims=True)

    with jax.named_scope("wait_ca"):
        receive(z_mate, z_order, ca, ca_r)
    carry_ref[...] = ca[...].reshape(8 * NR, 128)
    tiles = 2 * len(z_order) + len(x_order) + (1 + NR) * len(p_order)
    sent = l_ref.at[pl.ds(0, tiles * 8 // 2)]
    with jax.named_scope("wait_send"):
        pltpu.make_async_remote_copy(
            src_ref=sent, dst_ref=sent, send_sem=send_sem.at[0], recv_sem=z1_r.at[0],
            device_id=z_mate(1)[1], device_id_type=MESH).wait_send()
        sent = vq.at[pl.ds(0, len(q_order))]
        pltpu.make_async_remote_copy(
            src_ref=sent, dst_ref=sent, send_sem=vq_s.at[0], recv_sem=vq_r.at[0],
            device_id=z_mate(1)[1], device_id_type=MESH).wait_send()


def write_kernel(l_ref, e_ref, carry_ref, bt_ref, o_hbm, av, stage, sem):
    p = lax.axis_index("prow")
    q = lax.axis_index("pcol")
    src, dst = iota((128, B), 0), iota((128, B), 1)
    near = jnp.where((src % 4 == dst % 4) & ((src // 4 <= dst // 4) | (dst >= 128)), 1.0, 0.0).astype(BF16)
    scans = jnp.zeros((8 * NR, B), F32)
    for piece in split3(carry_ref[...]):
        scans = scans + dot(piece, near, ((1,), (0,)))
    av[...] = scans[:, :128].reshape(NR, 8, 128) + rows_before(scans[:, 128:].reshape(NR, 8, 128))

    cf = [[lax.rsqrt(((c * NX * NZ + q) * B + bt * 128 + 1 + iota((8, 128), 1)).astype(F32)) for bt in range(2)] for c in range(NC)]
    first_row = (p * B + 1 + iota((8, 128), 0) * STEPS).astype(F32)
    def row_block(r, _):
        carry = av[r]
        offset = {}
        for n in range(NI):
            for c in range(NC):
                own = e_ref[(n * NR + r) * NC + c]
                for bt in range(2):
                    offset[n, c, bt] = own[:, bt * 128:bt * 128 + 128] + bt_ref[r, pl.ds(n * 4 + bt * 2 + c, 1), :]
        for j in range(STEPS):
            rf = lax.rsqrt(first_row + (r * NP * B + j).astype(F32))
            scale = [[rf * cf[c][bt] for bt in range(2)] for c in range(NC)]
            for n in range(NI):
                k = n * NR + r
                for c in range(NC):
                    at = j * 4 + n * 2 + c
                    a = jnp.broadcast_to(carry[:, at:at + 1], (8, 128))
                    for bt in range(2):
                        lv = l_ref[pl.ds((k * NC + c) * B + j * 8, 8), pl.ds(bt * 128, 128)]
                        stage[pl.ds(k * 8 * PAD + j * 4 + c * 2 + bt, 8, stride=PAD), :] = (lv + (a + offset[n, c, bt])) * scale[c][bt]
        for n in range(NI):
            k = n * NR + r
            for i in range(8):
                pltpu.make_async_copy(
                    stage.at[pl.ds((k * 8 + i) * PAD, SEG)], o_hbm.at[pl.ds((k * 8 + i) * SEG, SEG)], sem.at[0]).start()
        return 0

    lax.fori_loop(0, NR, row_block, 0)
    pltpu.make_async_copy(stage.at[pl.ds(0, ROWS)], o_hbm, sem.at[0]).wait()


def shards(matrix):
    rows = matrix.reshape(NI, NR, B, NC, 2, 128).transpose(0, 1, 2, 4, 3, 5).reshape(ROWS, 128)
    rows = pltpu.with_memory_space_constraint(rows, pltpu.HBM)
    hbm = pl.BlockSpec(memory_space=pltpu.HBM)
    vmem = pl.BlockSpec(memory_space=pltpu.VMEM)
    dma = pltpu.SemaphoreType.DMA
    tile = lambda *lead: pltpu.VMEM((*lead, 8, 128), F32)
    found = pl.pallas_call(
        scan_kernel,
        out_shape=(
            pltpu.VMEM((BLOCKS * B, B), F32),
            pltpu.VMEM((BLOCKS, 8, B), F32),
            pltpu.VMEM((8 * NR, 128), F32),
            pltpu.VMEM((NR, 8, 128), F32),
        ),
        in_specs=[hbm],
        out_specs=(vmem, vmem, vmem, vmem),
        scratch_shapes=[
            pltpu.VMEM((ROWS, 128), BF16),
            pltpu.VMEM((2, 8 * PAD, 128), F32),
            tile(NR), tile(NR), tile(),
            tile(NZ), tile(NX), tile(NZ), tile(NZ), tile(),
            tile(NP), tile(NP, NR),
            pltpu.VMEM((1, 1, 128), F32), pltpu.VMEM((NX * NZ, 1, 128), F32), tile(NR),
            dma((GROUPS,)),
        ] + [dma((1,))] * 8,
        compiler_params=pltpu.CompilerParams(collective_id=0, has_side_effects=True, vmem_limit_bytes=24 << 20),
        name="scan",
    )(rows)
    out = pl.pallas_call(
        write_kernel,
        out_shape=pltpu.HBM((ROWS, 128), F32),
        in_specs=[vmem, vmem, vmem, vmem],
        out_specs=hbm,
        scratch_shapes=[tile(NR), pltpu.VMEM((NI * NR * 8 * PAD, 128), F32), dma((1,))],
        compiler_params=pltpu.CompilerParams(vmem_limit_bytes=24 << 20),
        name="write",
    )(*found)
    return out.reshape(NI, NR, 1, B, NC, 1, B)


def solution(mesh):
    return jax.shard_map(
        shards,
        mesh=mesh,
        in_specs=(P(None, None, "prow", None, None, "pcol", None),),
        out_specs=P(None, None, "prow", None, None, "pcol", None),
        check_vma=False,
    )
```
